128 devices in a mesh: rep: 4 (over z_hi, core), row: 4 (over x), col: 8 (over z_lo, y).
Axes of the slice: x: 4, y: 4, z: 4 (z_hi: 2, z_lo: 2; z = z_hi * 2 + z_lo), core: 2. Of those that a mesh axis runs over, the one named last changes fastest.
Arguments:
- grad_parts: bfloat16 [4, 16384, 6144], P('rep', ('row', 'col')), may hold values from -0.03125 to 0.03125, as said below
- statistic: float32 [6144, 6144], P('row', 'col'), may hold values from -150 to 150, as said below
Outputs:
- gram_matrix: float32 [6144, 6144], P('row', 'col')
- statistic_next: float32 [6144, 6144], P('row', 'col')
The draws below stay inside these ranges and needn't reach their ends.
Inputs may be any that keep to these rules, and one draw needn't show every extreme that they name: Every entry of grad_parts has a magnitude between 2^-10 and 2^-5. statistic is symmetric and positive definite.
All inputs are finite; a program needn't handle non-finite values.
Results may differ from the reference program's by a relative error of at most 0.008.
Values may be sent and summed in bfloat16 or wider, within the bound.
No kernel may reach another device: no remote copies, remote signals or barrier semaphores. Data moves between devices by JAX's collectives and lax.ppermute only.
A program may use at most 128 MiB of HBM per device.

```python
import math
import jax
import jax.numpy as jnp
from jax import lax

D = 6144
HID = 16384
N_REP = 4


def draw_grad_parts(key, part):
    key_sign = jax.random.fold_in(key, 41)
    key_level = jax.random.fold_in(key, 53)
    signs = jnp.where(jax.random.bernoulli(key_sign, 0.5, (N_REP, HID, D)), 1.0, -1.0).astype(jnp.float32)
    level = jax.random.uniform(key_level, (N_REP, HID, D), jnp.float32, -10.0, -5.0)
    return (signs * jnp.exp2(level)).astype(jnp.bfloat16)


def draw_statistic(key, part):
    key_factor = jax.random.fold_in(key, 11)
    key_ridge = jax.random.fold_in(key, 23)
    factor = jax.random.truncated_normal(key_factor, -3.0, 3.0, (D, D), jnp.float32) * (2.0 / math.sqrt(D))
    crossed = jnp.dot(factor.T, factor, precision=lax.Precision.HIGHEST)
    crossed = 0.5 * (crossed + crossed.T)
    ridge = jax.random.uniform(key_ridge, (D,), jnp.float32, 0.25, 1.0)
    return crossed + jnp.diag(ridge)


def setup_inputs(seed: int = 0) -> dict:
    seeds = jax.random.split(jax.random.key(seed), 3)
    grad_parts = draw_grad_parts(jax.random.fold_in(seeds[2], 71), 0)
    statistic = draw_statistic(jax.random.fold_in(seeds[2], 71), 0)
    return {"grad_parts": grad_parts, "statistic": statistic}


def reference(grad_parts, statistic):
    summed = jnp.sum(grad_parts.astype(jnp.float32), axis=0).astype(jnp.bfloat16)
    summed = lax.optimization_barrier(summed)
    summed_f32 = summed.astype(jnp.float32)
    product = jnp.dot(summed_f32.T, summed_f32, precision=lax.Precision.HIGHEST)
    gram_full = 0.5 * (product + product.T)
    statistic_next = 0.95 * statistic + 0.05 * gram_full
    return gram_full, statistic_next
```

```python
import jax
import jax.numpy as jnp
from jax import lax
from jax.sharding import Mesh, PartitionSpec as P

CHUNKS = 2
F32, BF16 = jnp.float32, jnp.bfloat16


def shift(v, axis, step):
    n = lax.axis_size(axis)
    return lax.ppermute(v, axis, [(i, (i + step) % n) for i in range(n)])


def spread(block, axis):
    up, down = shift(block, axis, 1), shift(block, axis, -1)
    far_low, far_high = shift(up[:2], axis, 1), shift(down[2:], axis, -1)
    return block, up, jnp.concatenate([far_low, far_high]), down


def shards(grad_parts, statistic):
    part = grad_parts[0]
    rows, width = part.shape[0] // (4 * CHUNKS), part.shape[1] // 8
    zh, c, x, zl, y = (lax.axis_index(a) for a in ("zh", "c", "x", "zl", "y"))
    part = part.reshape(2, 2, CHUNKS, rows, 8, width).transpose(4, 0, 1, 2, 3, 5)
    mine = lax.dynamic_index_in_dim(part, c, 1, keepdims=False)
    theirs = lax.dynamic_index_in_dim(part, 1 - c, 1, keepdims=False)
    total = None
    paired = [
        mine[:, :, k].astype(F32) + shift(theirs[:, :, k], "c", 1).astype(F32)
        for k in range(CHUNKS)
    ]
    arrived = [
        shift(lax.dynamic_index_in_dim(p, 1 - zh, 1, keepdims=False).astype(BF16), "zh", 1)
        for p in paired
    ]
    for k in range(CHUNKS):
        kept = lax.dynamic_index_in_dim(paired[k], zh, 1, keepdims=False)
        summed = (kept + arrived[k].astype(F32)).astype(BF16)
        by_row = summed.reshape(4, 2, rows, width)
        by_col = summed.reshape(2, 4, rows, width)
        by_col = jnp.stack([by_col[0], by_col[1]])
        by_col = jnp.where(c == 0, by_col, by_col[::-1])
        lefts, rights = [], []
        for d in range(4):
            piece = lax.dynamic_index_in_dim(by_row, (x + d) % 4, 0, keepdims=False)
            lefts.append(shift(piece, "x", d) if d else piece)
            piece = lax.dynamic_index_in_dim(by_col, (y + d) % 4, 1, keepdims=False)
            rights.append(shift(piece, "y", d) if d else piece)
        left = spread(jnp.stack(lefts), "y")
        right = spread(jnp.stack(rights), "x")
        tile = []
        for j in range(2):
            r = jnp.concatenate([right[d][e, j] for e in range(4) for d in range(4)])
            column = []
            for i in range(2):
                l = jnp.concatenate([left[e][d, i] for e in range(4) for d in range(4)])
                column.append(lax.dot_general(l, r, (((0,), (0,)), ((), ())), preferred_element_type=F32))
            tile.append(jnp.stack(column))
        total = tile if total is None else [a + b for a, b in zip(total, tile)]
    own = total[0] + shift(total[1].astype(BF16), "c", 1).astype(F32)
    half = own.astype(BF16)
    line = ("zh", "c", "zl")

    def at(z, core):
        return (z // 2) * 4 + core * 2 + z % 2

    roots = [(z, core) for z in range(4) for core in range(2) if z % 2 == core]
    others = [(z, core) for z in range(4) for core in range(2) if z % 2 != core]
    across = [(at(z, k), at((z + 2) % 4, k)) for z, k in roots]
    pick = lambda h: lax.dynamic_index_in_dim(half, h, 0, keepdims=False)
    above = ((2 * zh + zl + 1) % 4) // 2
    below = ((2 * zh + zl + 3) % 4) // 2
    got = lax.ppermute(pick(1 - zh), line, across).astype(F32)
    got += lax.ppermute(pick(above), line, [(at(z, k), at((z + 1) % 4, k)) for z, k in others]).astype(F32)
    got += lax.ppermute(pick(below), line, [(at(z, k), at((z + 3) % 4, k)) for z, k in others]).astype(F32)
    near = (lax.dynamic_index_in_dim(own, zh, 0, keepdims=False) + got).astype(BF16)
    far = lax.ppermute(near, line, across)
    sideways = [(at(z, k), at(z, 1 - k)) for z, k in roots]
    near_in, far_in = lax.ppermute(near, line, sideways), lax.ppermute(far, line, sideways)
    root = zl == c
    near, far = jnp.where(root, near, near_in), jnp.where(root, far, far_in)
    gram = jnp.concatenate([jnp.where(zh == 0, near, far), jnp.where(zh == 0, far, near)]).astype(F32)
    return gram, 0.95 * statistic + 0.05 * gram


def solution(mesh):
    fine = Mesh(mesh.devices.reshape(2, 2, 4, 2, 4), ("zh", "c", "x", "zl", "y"))
    return jax.shard_map(
        shards,
        mesh=fine,
        in_specs=(P(("zh", "c"), ("x", "zl", "y"), None), P("x", ("zl", "y"))),
        out_specs=(P("x", ("zl", "y")), P("x", ("zl", "y"))),
        check_vma=False,
    )
```

```python
import jax
import jax.numpy as jnp
from jax import lax
from jax.experimental import pallas as pl
from jax.experimental.pallas import tpu as pltpu
from jax.sharding import Mesh, PartitionSpec as P

STEPS = 3
SHARES = (1, 1)
F32, BF16 = jnp.float32, jnp.bfloat16
VMEM = pl.BlockSpec(memory_space=pltpu.VMEM)
SMEM = pl.BlockSpec(memory_space=pltpu.SMEM)
HBM = pl.BlockSpec(memory_space=pltpu.HBM)


def shift(v, axis, step):
    n = lax.axis_size(axis)
    return lax.ppermute(v, axis, [(i, (i + step) % n) for i in range(n)])


def shift_z(v, step):
    return lax.ppermute(v, ("zh", "zl"), [(i, (i + step) % 4) for i in range(4)])


def after(v, *others):
    return lax.optimization_barrier((v, *others))[0]


def slab(v, start, size):
    return lax.dynamic_slice_in_dim(v, start, size)


def params(mib):
    return pltpu.CompilerParams(vmem_limit_bytes=mib * 2**20)


def cost(flops):
    return pl.CostEstimate(flops=flops, bytes_accessed=10**6, transcendentals=0)


def scalars(*values):
    return jnp.stack(values).astype(jnp.int32)


def sum_kernel(at, own, beside, across, *refs):
    lefts, rights, (total,) = refs[:4], refs[4:8], refs[8:]
    width = own.shape[1] // 8
    c, x, y = at[0], at[1], at[2]
    total[...] = (own[...].astype(F32) + beside[...].astype(F32) + across[...].astype(F32)).astype(BF16)
    for d in range(4):
        for i in range(2):
            block = lax.rem(x + d, 4) * 2 + (i + c - 2 * i * c)
            lefts[d][i] = total[:, pl.ds(pl.multiple_of(block * width, width), width)]
            block = lax.rem(y + d, 4) + 4 * i
            rights[d][i] = total[:, pl.ds(pl.multiple_of(block * width, width), width)]


def sum_and_split(at, own, beside, across):
    rows, width = across.shape[0], across.shape[1] // 8
    piece = jax.ShapeDtypeStruct((2, rows, width), BF16)
    return pl.pallas_call(
        sum_kernel,
        out_shape=[piece] * 8,
        in_specs=[SMEM, VMEM, VMEM, VMEM],
        out_specs=[VMEM] * 8,
        scratch_shapes=[pltpu.VMEM(across.shape, BF16)],
        compiler_params=params(8),
        cost_estimate=cost(10**9),
        name="sum_and_split",
    )(at, own, beside, across)


def panel_kernel(*refs):
    lefts, rights, (left, right) = refs[:5], refs[5:10], refs[10:]
    rows, width = lefts[0].shape[2:]
    for e in range(4):
        for d in range(4):
            l, r = (
                p[e].at[d] if e < 2 else p[4].at[d] if e == 3 else p[2 + d // 2].at[d % 2] for p in (lefts, rights)
            )
            for i in range(2):
                left[i, pl.ds((e * 4 + d) * rows, rows)] = l[i]
                right[pl.ds((d * 4 + e) * rows, rows), pl.ds(i * width, width)] = r[i]


def panels(lefts, rights):
    rows, width = lefts[0].shape[2:]
    depth = 16 * rows
    return pl.pallas_call(
        panel_kernel,
        out_shape=[
            jax.ShapeDtypeStruct((2, depth, width), BF16),
            jax.ShapeDtypeStruct((depth, 2 * width), BF16),
        ],
        in_specs=[VMEM] * 10,
        out_specs=[VMEM] * 2,
        compiler_params=params(16),
        cost_estimate=cost(10**9),
        name="panels",
    )(*lefts, *rights)


def gather(pieces, axis):
    mine = jnp.stack(pieces)
    up, down = shift(mine, axis, 1), shift(mine, axis, -1)
    low, high = shift(up[:2], axis, 1), shift(down[2:], axis, -1)
    return [mine, up, low, high, down]


def merge_kernel(at, own, other, opposite, above, below, mine):
    rows, cols = mine.shape

    def quarter(row, col):
        rs = pl.ds(pl.multiple_of(row * rows, 16), rows)
        cs = pl.ds(pl.multiple_of(col * cols, cols), cols)
        return own[rs, cs] + other[rs, cs].astype(F32)

    zh, zl = at[0], at[1]
    opposite[...] = quarter(1 - zh, zl).astype(BF16)
    above[...] = quarter(at[2], 1 - zl).astype(BF16)
    below[...] = quarter(at[3], 1 - zl).astype(BF16)
    mine[...] = quarter(zh, zl)


def merge(at, own, other):
    rows, cols = own.shape
    sent = jax.ShapeDtypeStruct((rows // 2, cols // 2), BF16)
    return pl.pallas_call(
        merge_kernel,
        out_shape=[sent, sent, sent, jax.ShapeDtypeStruct(sent.shape, F32)],
        in_specs=[SMEM, VMEM, VMEM],
        out_specs=[VMEM] * 4,
        compiler_params=params(16),
        cost_estimate=cost(10**9),
        name="merge",
    )(at, own, other)


def finish_kernel(at, here, beside, statistic, *refs):
    gram, following = refs[-2:]
    mine = pl.program_id(0) // (pl.num_programs(0) // 2) == at[1]
    value = jnp.where(mine, here[...].astype(F32), beside[...].astype(F32))
    gram[...] = value
    following[...] = 0.95 * statistic[...] + 0.05 * value


def finish(at, here, beside, statistic, made):
    rows, cols = here.shape
    n = STEPS if rows % (16 * STEPS) == 0 else 1
    small = pl.BlockSpec((rows // n, cols), lambda t, at: (t % n, 0))
    taken = pl.BlockSpec((rows // n, cols), lambda t, at: (t, 0))
    block = pl.BlockSpec((rows // n, cols), lambda t, at: ((t // n * 2 + at[0]) * n + t % n, 0))
    return pl.pallas_call(
        finish_kernel,
        grid_spec=pltpu.PrefetchScalarGridSpec(
            num_scalar_prefetch=1,
            grid=(2 * n,),
            in_specs=[small, small, taken] + [HBM] * len(made),
            out_specs=[block] * 2,
        ),
        out_shape=[jax.ShapeDtypeStruct((4 * rows, cols), F32)] * 2,
        input_output_aliases={4: 0, 5: 1} if made else {},
        compiler_params=params(8),
        cost_estimate=cost(10**9),
        name="finish",
    )(at, here, beside, statistic, *made)


def product(left, right):
    return lax.dot_general(left, right, (((0,), (0,)), ((), ())), preferred_element_type=F32)


def shards(grad_parts, statistic):
    part = grad_parts[0]
    width = part.shape[1] // 8
    zh, c, x, zl, y = (lax.axis_index(a) for a in ("zh", "c", "x", "zl", "y"))
    at = scalars(c, x, y)
    half = part.shape[0] // 2
    sizes = [half // 2 * s // sum(SHARES) for s in SHARES]
    bases = [2 * sum(sizes[:k]) for k in range(len(sizes))]
    beside, gate = [], part
    for size, base in zip(sizes, bases):
        theirs = slab(gate, (1 - c) * half + base, 2 * size)
        beside.append(shift(theirs, "c", 1))
        gate = after(part, theirs)
    sent, across = [], []
    for k, (size, base) in enumerate(zip(sizes, bases)):
        mine = slab(after(part, *sent), c * half + base + (1 - zh) * size, size)
        theirs = slab(beside[k], (1 - zh) * size, size)
        sent.append((mine.astype(F32) + theirs.astype(F32)).astype(BF16))
        across.append(shift(sent[-1], "zh", 1))
    wide = after(statistic, *sent).reshape(2, 2, width // 2, width)
    near_stat, far_stat = (
        lax.dynamic_index_in_dim(wide, h, 1, keepdims=False).reshape(width, width) for h in (zh, 1 - zh)
    )
    owns = []
    for size, base in zip(sizes, bases):
        owns.append(slab(after(part, *sent, *owns), c * half + base + zh * size, size))
    across[0] = after(across[0], *sent[1:], near_stat, far_stat, *owns)
    totals, lefts, rights = [None, None], [], []
    for k, size in enumerate(sizes):
        theirs = slab(after(beside[k], *sent), zh * size, size)
        pieces = sum_and_split(at, owns[k], theirs, after(across[k], *lefts, *rights))
        lefts, rights = list(pieces[:4]), list(pieces[4:])
        for d in (1, 3, 2):
            lefts[d] = shift(lefts[d], "x", d)
            rights[d] = shift(rights[d], "y", d)
        parts = gather(lefts, "y") + gather(rights, "x")
        if k:
            parts = lax.optimization_barrier((parts, totals))[0]
        left, right = panels(parts[:5], parts[5:])
        if k + 1 < len(sizes):
            for i in range(2):
                p = product(left[i], right)
                totals[i] = p if totals[i] is None else p + totals[i]

    def last(i, left):
        p = product(left[i], right)
        return p if totals[i] is None else p + totals[i]

    other = last(1, left).astype(BF16)
    own = last(0, after(left, other))
    other = shift(other, "c", 1)
    above, below = ((2 * zh + zl + s) % 4 // 2 for s in (1, 3))
    opposite, above, below, mine = merge(scalars(zh, zl, above, below), own, other)
    got = shift(opposite, "zh", 1).astype(F32)
    got += shift_z(above, 1).astype(F32)
    got += shift_z(below, -1).astype(F32)
    near = (mine + got).astype(BF16)
    near_in = shift(near, "c", 1)
    far = shift(near, "zh", 1)
    far_in = shift(far, "c", 1)
    made = finish(scalars(zh, c), near, near_in, near_stat, ())
    return tuple(finish(scalars(1 - zh, c), far, far_in, far_stat, made))


def solution(mesh):
    fine = Mesh(mesh.devices.reshape(2, 2, 4, 2, 4), ("zh", "c", "x", "zl", "y"))
    return jax.shard_map(
        shards,
        mesh=fine,
        in_specs=(P(("zh", "c"), ("x", "zl", "y"), None), P("x", ("zl", "y"))),
        out_specs=(P("x", ("zl", "y")), P("x", ("zl", "y"))),
        check_vma=False,
    )
```

```python
import functools

import jax
import jax.numpy as jnp
from jax import lax
from jax.experimental import pallas as pl
from jax.experimental.pallas import tpu as pltpu
from jax.sharding import Mesh, PartitionSpec as P

STEPS, TILES = 1, 3
SHARES = (1, 1)
F32, BF16 = jnp.float32, jnp.bfloat16
VMEM = pl.BlockSpec(memory_space=pltpu.VMEM)
SMEM = pl.BlockSpec(memory_space=pltpu.SMEM)
HBM = pl.BlockSpec(memory_space=pltpu.HBM)


def shift(v, axis, step):
    n = lax.axis_size(axis)
    return lax.ppermute(v, axis, [(i, (i + step) % n) for i in range(n)])


def shift_z(v, step):
    return lax.ppermute(v, ("zh", "zl"), [(i, (i + step) % 4) for i in range(4)])


def after(v, *others):
    return lax.optimization_barrier((v, *others))[0]


def slab(v, start, size):
    return lax.dynamic_slice_in_dim(v, start, size)


def params(mib):
    return pltpu.CompilerParams(vmem_limit_bytes=mib * 2**20)


def cost(flops):
    return pl.CostEstimate(flops=flops, bytes_accessed=10**6, transcendentals=0)


def flip(bit, other):
    return bit + other - 2 * bit * other


def sum_kernel(at, own, beside, across, *refs):
    lefts, rights, (total,) = refs[:4], refs[4:8], refs[8:]
    width = own.shape[1] // 8
    c, x, y = at[0], at[1], at[2]
    total[...] = (own[...].astype(F32) + beside[...].astype(F32) + across[...].astype(F32)).astype(BF16)
    for d in range(4):
        for i in range(2):
            block = lax.rem(x + d, 4) * 2 + flip(i, c)
            lefts[d][i] = total[:, pl.ds(pl.multiple_of(block * width, width), width)]
            block = lax.rem(y + d, 4) + 4 * i
            rights[d][i] = total[:, pl.ds(pl.multiple_of(block * width, width), width)]


def sum_and_split(at, own, beside, across):
    rows, width = across.shape[0], across.shape[1] // 8
    piece = jax.ShapeDtypeStruct((2, rows, width), BF16)
    return pl.pallas_call(
        sum_kernel,
        out_shape=[piece] * 8,
        in_specs=[SMEM, VMEM, VMEM, VMEM],
        out_specs=[VMEM] * 8,
        scratch_shapes=[pltpu.VMEM(across.shape, BF16)],
        compiler_params=params(8),
        cost_estimate=cost(10**9),
        name="sum_and_split",
    )(at, own, beside, across)


def piece_at(p, e, d):
    if len(p) == 8:
        return p[2 * e + d // 2].at[d % 2]
    return p[2 + d // 2].at[d % 2] if e == 2 else p[min(e, 2) + 2 * (e == 3)].at[d]


def panel_kernel(*refs):
    n = len(refs) // 2 - 1
    lefts, rights, (left, right) = refs[:n], refs[n : 2 * n], refs[2 * n :]
    rows, width = lefts[0].shape[2:]
    for e in range(4):
        for d in range(4):
            l, r = piece_at(lefts, e, d), piece_at(rights, e, d)
            for i in range(2):
                left[i, pl.ds((e * 4 + d) * rows, rows)] = l[i]
                right[pl.ds((d * 4 + e) * rows, rows), pl.ds(i * width, width)] = r[i]


def panels(lefts, rights):
    rows, width = lefts[0].shape[2:]
    depth = 16 * rows
    return pl.pallas_call(
        panel_kernel,
        out_shape=[
            jax.ShapeDtypeStruct((2, depth, width), BF16),
            jax.ShapeDtypeStruct((depth, 2 * width), BF16),
        ],
        in_specs=[VMEM] * (len(lefts) + len(rights)),
        out_specs=[VMEM] * 2,
        compiler_params=params(2),
        cost_estimate=cost(10**9),
        name="panels",
    )(*lefts, *rights)


def gather(pieces, axis, split):
    if split:
        low, high = jnp.stack(pieces[:2]), jnp.stack(pieces[2:])
        up_low, down_high = shift(low, axis, 1), shift(high, axis, -1)
        up_high, down_low = shift(high, axis, 1), shift(low, axis, -1)
        far_low, far_high = shift(up_low, axis, 1), shift(down_high, axis, -1)
        return [low, high, up_low, up_high, far_low, far_high, down_low, down_high]
    mine = jnp.stack(pieces)
    up, down = shift(mine, axis, 1), shift(mine, axis, -1)
    low, high = shift(up[:2], axis, 1), shift(down[2:], axis, -1)
    return [mine, up, low, high, down]


def merge_kernel(at, own, other, *refs):
    rows, cols = refs[0].shape
    zh, zl = at[3], at[4]
    quarters = (1 - zh, zl), (flip(zh, zl), 1 - zl), (flip(zh, 1 - zl), 1 - zl), (zh, zl)
    for k, (row, col) in enumerate(quarters):
        rs = pl.ds(pl.multiple_of(row * rows, 16), rows)
        for h in range(2):
            cs = pl.ds(pl.multiple_of(col * (2 * cols) + h * cols, cols), cols)
            out = refs[2 * k + h]
            out[...] = (own[rs, cs] + other[rs, cs].astype(F32)).astype(out.dtype)


def merge(at, own, other):
    rows, cols = own.shape
    shape = (rows // 2, cols // 4)
    kinds = (BF16, BF16), (BF16, F32), (F32, BF16), (F32, F32)
    return pl.pallas_call(
        merge_kernel,
        out_shape=[jax.ShapeDtypeStruct(shape, kind) for pair in kinds for kind in pair],
        in_specs=[SMEM, VMEM, VMEM],
        out_specs=[VMEM] * 8,
        compiler_params=params(6),
        cost_estimate=cost(10**9),
        name="merge",
    )(at, own, other)


def finish_kernel(cs, at, here, beside, statistic, *refs):
    gram, following = refs[-2:]
    t, n = pl.program_id(0), pl.num_programs(0) // 2
    rows = gram.shape[0]
    there = pl.ds(pl.multiple_of(lax.rem(t, n) * rows, 16), rows)
    value = jnp.where(t // n == at[0], here[there, :], beside[there, :]).astype(F32)
    gram[...] = value
    following[...] = 0.95 * statistic[pl.ds(pl.multiple_of(t * rows, 16), rows), cs] + 0.05 * value


def finish(at, far, q, here, beside, statistic, made):
    rows, cols = here.shape
    n = STEPS if rows % (16 * STEPS) == 0 else 1
    block = pl.BlockSpec((rows // n, cols), lambda t, at: ((t // n * 2 + flip(at[3], far)) * n + t % n, q))
    return pl.pallas_call(
        functools.partial(finish_kernel, pl.ds(q * cols, cols)),
        grid_spec=pltpu.PrefetchScalarGridSpec(
            num_scalar_prefetch=1,
            grid=(2 * n,),
            in_specs=[VMEM] * 3 + [HBM] * len(made),
            out_specs=[block] * 2,
        ),
        out_shape=[jax.ShapeDtypeStruct((4 * rows, statistic.shape[1]), F32)] * 2,
        input_output_aliases={4: 0, 5: 1} if made else {},
        compiler_params=params(8),
        cost_estimate=cost(10**9),
        name="finish",
    )(at, here, beside, statistic, *made)


def product_kernel(i, left, right, *refs):
    out = refs[-1]
    rows, cols = out.shape[0] // TILES, out.shape[1] // 2

    @pl.loop(0, TILES)
    def _(t):
        rs = pl.ds(pl.multiple_of(t * rows, rows), rows)
        for j in range(2):
            cs = pl.ds(j * cols, cols)
            p = lax.dot_general(left[i, :, rs], right[:, cs], (((0,), (0,)), ((), ())), preferred_element_type=F32)
            out[rs, cs] = (p if len(refs) == 1 else p + refs[0][rs, cs]).astype(out.dtype)


def product(i, left, right, before, dtype):
    rows, cols = left.shape[2], right.shape[1]
    given = [left, right] + ([] if before is None else [before])
    return pl.pallas_call(
        functools.partial(product_kernel, i),
        in_specs=[VMEM] * len(given),
        out_specs=VMEM,
        out_shape=jax.ShapeDtypeStruct((rows, cols), dtype),
        compiler_params=params(6),
        cost_estimate=cost(2 * left.shape[1] * rows * cols),
        name="product",
    )(*given)


def shards(grad_parts, statistic):
    part = grad_parts[0]
    width = part.shape[1] // 8
    zh, c, x, zl, y = (lax.axis_index(a) for a in ("zh", "c", "x", "zl", "y"))
    at = jnp.stack([c, x, y, zh, zl]).astype(jnp.int32)
    half = part.shape[0] // 2
    sizes = [half // 2 * s // sum(SHARES) for s in SHARES]
    bases = [2 * sum(sizes[:k]) for k in range(len(sizes))]
    beside, gate = [], part
    for size, base in zip(sizes, bases):
        theirs = slab(gate, (1 - c) * half + base, 2 * size)
        beside.append(shift(theirs, "c", 1))
        gate = after(part, theirs)
    sent, across = [], []
    for k, (size, base) in enumerate(zip(sizes, bases)):
        mine = slab(after(part, *sent), c * half + base + (1 - zh) * size, size)
        theirs = slab(beside[k], (1 - zh) * size, size)
        sent.append((mine.astype(F32) + theirs.astype(F32)).astype(BF16))
        across.append(shift(sent[-1], "zh", 1))
    wide = after(statistic, *sent).reshape(2, 2, width // 2, width)
    near_stat, far_stat = (
        lax.dynamic_index_in_dim(wide, h, 1, keepdims=False).reshape(width, width) for h in (zh, 1 - zh)
    )
    owns = []
    for size, base in zip(sizes, bases):
        owns.append(slab(after(part, *sent, *owns), c * half + base + zh * size, size))
    across[0] = after(across[0], *sent[1:], near_stat, far_stat, *owns)
    totals, lefts, rights = [None, None], [], []
    for k, size in enumerate(sizes):
        theirs = slab(after(beside[k], *sent), zh * size, size)
        pieces = sum_and_split(at, owns[k], theirs, after(across[k], *lefts, *rights))
        lefts, rights = list(pieces[:4]), list(pieces[4:])
        for d in (1, 3, 2):
            lefts[d] = shift(lefts[d], "x", d)
            rights[d] = shift(rights[d], "y", d)
        split = k + 1 == len(sizes)
        parts = gather(lefts, "y", split), gather(rights, "x", split)
        if k:
            parts = lax.optimization_barrier((parts, totals))[0]
        left, right = panels(*parts)
        if k + 1 < len(sizes):
            for i in range(2):
                totals[i] = product(i, left, right, totals[i], F32)
    other = product(1, left, right, totals[1], BF16)
    other = shift(other, "c", 1)
    own = product(0, left, right, totals[0], F32)
    low, high, above_low, above_high, below_low, below_high, *mine = merge(at, own, other)
    low, high = shift_z(low, -1), shift_z(high, 1)
    above_low, below_high = shift_z(above_low, 1), shift_z(below_high, -1)
    below_low = shift_z((below_low + low.astype(F32)).astype(BF16), -1)
    above_high = shift_z((above_high + high.astype(F32)).astype(BF16), 1)
    pairs = (above_low, below_low), (above_high, below_high)
    near = [(m + a.astype(F32) + b.astype(F32)).astype(BF16) for m, (a, b) in zip(mine, pairs)]
    far, made = [], ()
    for q in range(2):
        beside = shift(near[q], "c", 1)
        far.append(shift(near[q], "zh", 1))
        made = finish(at, 0, q, near[q], beside, near_stat, made)
    for q in range(2):
        beside = shift(far[q], "c", 1)
        made = finish(at, 1, q, far[q], beside, far_stat, made)
    return tuple(made)


def solution(mesh):
    fine = Mesh(mesh.devices.reshape(2, 2, 4, 2, 4), ("zh", "c", "x", "zl", "y"))
    return jax.shard_map(
        shards,
        mesh=fine,
        in_specs=(P(("zh", "c"), ("x", "zl", "y"), None), P("x", ("zl", "y"))),
        out_specs=(P("x", ("zl", "y")), P("x", ("zl", "y"))),
        check_vma=False,
    )
```

```python
import functools

import jax
import jax.numpy as jnp
from jax import lax
from jax.experimental import pallas as pl
from jax.experimental.pallas import tpu as pltpu
from jax.sharding import Mesh, PartitionSpec as P

THIRDS = 1, 1, 1
SHARES = (1, 1)
F32, BF16 = jnp.float32, jnp.bfloat16
VMEM = pl.BlockSpec(memory_space=pltpu.VMEM)
SMEM = pl.BlockSpec(memory_space=pltpu.SMEM)
HBM = pl.BlockSpec(memory_space=pltpu.HBM)


def shift(v, axis, step):
    n = lax.axis_size(axis)
    return lax.ppermute(v, axis, [(i, (i + step) % n) for i in range(n)])


def shift_z(v, step):
    return lax.ppermute(v, ("zh", "zl"), [(i, (i + step) % 4) for i in range(4)])


def after(v, *others):
    return lax.optimization_barrier((v, *others))[0]


def slab(v, start, size):
    return lax.dynamic_slice_in_dim(v, start, size)


def params(mib):
    return pltpu.CompilerParams(vmem_limit_bytes=mib * 2**20)


def cost(flops):
    return pl.CostEstimate(flops=flops, bytes_accessed=10**6, transcendentals=0)


def flip(bit, other):
    return bit + other - 2 * bit * other


def sum_kernel(at, own, beside, across, *refs):
    lefts, rights, (total,) = refs[:4], refs[4:8], refs[8:]
    width = own.shape[1] // 8
    c, x, y = at[0], at[1], at[2]
    total[...] = (own[...].astype(F32) + beside[...].astype(F32) + across[...].astype(F32)).astype(BF16)
    for d in range(4):
        for i in range(2):
            block = lax.rem(x + d, 4) * 2 + flip(i, c)
            lefts[d][i] = total[:, pl.ds(pl.multiple_of(block * width, width), width)]
            block = lax.rem(y + d, 4) + 4 * i
            rights[d][i] = total[:, pl.ds(pl.multiple_of(block * width, width), width)]


def sum_and_split(at, own, beside, across):
    rows, width = across.shape[0], across.shape[1] // 8
    piece = jax.ShapeDtypeStruct((2, rows, width), BF16)
    return pl.pallas_call(
        sum_kernel,
        out_shape=[piece] * 8,
        in_specs=[SMEM, VMEM, VMEM, VMEM],
        out_specs=[VMEM] * 8,
        scratch_shapes=[pltpu.VMEM(across.shape, BF16)],
        compiler_params=params(8),
        cost_estimate=cost(10**9),
        name="sum_and_split",
    )(at, own, beside, across)


def piece_at(p, e, d):
    if len(p) == 8:
        return p[2 * e + d // 2].at[d % 2]
    return p[2 + d // 2].at[d % 2] if e == 2 else p[min(e, 2) + 2 * (e == 3)].at[d]


def panel_kernel(*refs):
    n = len(refs) // 2 - 1
    lefts, rights, (left, right) = refs[:n], refs[n : 2 * n], refs[2 * n :]
    rows, width = lefts[0].shape[2:]
    for e in range(4):
        for d in range(4):
            l, r = piece_at(lefts, e, d), piece_at(rights, e, d)
            for i in range(2):
                left[i, pl.ds((e * 4 + d) * rows, rows)] = l[i]
                right[pl.ds((d * 4 + e) * rows, rows), pl.ds(i * width, width)] = r[i]


def panels(lefts, rights):
    rows, width = lefts[0].shape[2:]
    depth = 16 * rows
    return pl.pallas_call(
        panel_kernel,
        out_shape=[
            jax.ShapeDtypeStruct((2, depth, width), BF16),
            jax.ShapeDtypeStruct((depth, 2 * width), BF16),
        ],
        in_specs=[VMEM] * (len(lefts) + len(rights)),
        out_specs=[VMEM] * 2,
        compiler_params=params(2),
        cost_estimate=cost(10**9),
        name="panels",
    )(*lefts, *rights)


def gather(pieces, axis, split):
    if split:
        low, high = jnp.stack(pieces[:2]), jnp.stack(pieces[2:])
        up_low, down_high = shift(low, axis, 1), shift(high, axis, -1)
        up_high, down_low = shift(high, axis, 1), shift(low, axis, -1)
        far_low, far_high = shift(up_low, axis, 1), shift(down_high, axis, -1)
        return [low, high, up_low, up_high, far_low, far_high, down_low, down_high]
    mine = jnp.stack(pieces)
    up, down = shift(mine, axis, 1), shift(mine, axis, -1)
    low, high = shift(up[:2], axis, 1), shift(down[2:], axis, -1)
    return [mine, up, low, high, down]


def merge_kernel(at, own, other, *refs):
    rows, cols = refs[0].shape
    for k, row in enumerate((flip(at[3], at[4]), flip(at[3], 1 - at[4]))):
        rs = pl.ds(pl.multiple_of(row * rows, 16), rows)
        for h in range(2):
            cs = pl.ds(h * cols, cols)
            out = refs[2 * k + h]
            out[...] = (own[rs, cs] + other[rs, cs].astype(F32)).astype(out.dtype)


def merge(at, own, other):
    rows, cols = own.shape
    kinds = BF16, F32, F32, BF16
    return pl.pallas_call(
        merge_kernel,
        out_shape=[jax.ShapeDtypeStruct((rows // 2, cols // 2), kind) for kind in kinds],
        in_specs=[SMEM, VMEM, VMEM],
        out_specs=[VMEM] * 4,
        compiler_params=params(6),
        cost_estimate=cost(10**9),
        name="merge",
    )(at, own, other)


def close_kernel(own, other, above_low, below_low, above_high, below_high, *outs):
    cols = above_low.shape[1]
    first = 0
    for out in outs:
        rs = pl.ds(first, out.shape[0])
        for h, (above, below) in enumerate(((above_low, below_low), (above_high, below_high))):
            cs = pl.ds(h * cols, cols)
            total = own[rs, cs] + other[rs, cs].astype(F32) + above[rs, :].astype(F32) + below[rs, :].astype(F32)
            out[:, cs] = total.astype(BF16)
        first += out.shape[0]


def close(sizes, own, other, *pieces):
    return pl.pallas_call(
        close_kernel,
        out_shape=[jax.ShapeDtypeStruct((size, own.shape[1]), BF16) for size in sizes],
        in_specs=[VMEM] * (2 + len(pieces)),
        out_specs=[VMEM] * len(sizes),
        compiler_params=params(4),
        cost_estimate=cost(10**9),
        name="close",
    )(own, other, *pieces)


def finish_kernel(first, at, here, beside, statistic, *refs):
    gram, following = refs[-2:]
    t, n = pl.program_id(0), pl.num_programs(0) // 2
    rows = gram.shape[0]
    r = lax.rem(t, n)
    there = pl.ds(pl.multiple_of(r * rows, 16), rows)
    old = pl.ds(pl.multiple_of(t // n * (statistic.shape[0] // 2) + (first + r) * rows, 16), rows)
    value = jnp.where(t // n == at[0], here[there, :], beside[there, :]).astype(F32)
    gram[...] = value
    following[...] = 0.95 * statistic[old, :] + 0.05 * value


def finish(at, far, first, here, beside, statistic, made):
    cols = here.shape[1]
    rows = statistic.shape[0] // 2 // sum(THIRDS)
    n = here.shape[0] // rows
    block = pl.BlockSpec(
        (rows, cols), lambda t, at: ((t // n * 2 + flip(at[3], far)) * sum(THIRDS) + first + t % n, 0)
    )
    return pl.pallas_call(
        functools.partial(finish_kernel, first),
        grid_spec=pltpu.PrefetchScalarGridSpec(
            num_scalar_prefetch=1,
            grid=(2 * n,),
            in_specs=[VMEM] * 3 + [HBM] * len(made),
            out_specs=[block] * 2,
        ),
        out_shape=[jax.ShapeDtypeStruct((2 * statistic.shape[0], cols), F32)] * 2,
        input_output_aliases={4: 0, 5: 1} if made else {},
        compiler_params=params(8),
        cost_estimate=cost(10**9),
        name="finish",
    )(at, here, beside, statistic, *made)


def product_kernel(i, cut, at, left, right, *refs):
    before, out = refs[:-1], refs[-1]
    width = left.shape[2]
    step = width // 2
    row, col = cut

    def span(base, k, size):
        return pl.ds(k * size, size) if base is None else pl.ds(pl.multiple_of(base * size, size), size)

    for k in range(out.shape[0] // step):
        rs = span(None if row is None else flip(at[3], row), k, step)
        for m in range(out.shape[1] // width):
            cs = span(None if col is None else flip(at[4], col), m, width)
            p = lax.dot_general(left[i, :, rs], right[:, cs], (((0,), (0,)), ((), ())), preferred_element_type=F32)
            for b in before:
                p += b[rs, cs]
            out[pl.ds(k * step, step), pl.ds(m * width, width)] = p.astype(out.dtype)


def product(i, cut, at, left, right, before, dtype):
    rows, cols = left.shape[2] // (1 if cut[0] is None else 2), right.shape[1] // (1 if cut[1] is None else 2)
    given = [left, right] + ([] if before is None else [before])
    return pl.pallas_call(
        functools.partial(product_kernel, i, cut),
        in_specs=[SMEM] + [VMEM] * len(given),
        out_specs=VMEM,
        out_shape=jax.ShapeDtypeStruct((rows, cols), dtype),
        compiler_params=params(6),
        cost_estimate=cost(2 * left.shape[1] * rows * cols),
        name="product",
    )(at, *given)


def shards(grad_parts, statistic):
    part = grad_parts[0]
    width = part.shape[1] // 8
    zh, c, x, zl, y = (lax.axis_index(a) for a in ("zh", "c", "x", "zl", "y"))
    at = jnp.stack([c, x, y, zh, zl]).astype(jnp.int32)
    half = part.shape[0] // 2
    sizes = [half // 2 * s // sum(SHARES) for s in SHARES]
    bases = [2 * sum(sizes[:k]) for k in range(len(sizes))]
    beside, gate = [], part
    for size, base in zip(sizes, bases):
        theirs = slab(gate, (1 - c) * half + base, 2 * size)
        beside.append(shift(theirs, "c", 1))
        gate = after(part, theirs)
    sent, across = [], []
    for k, (size, base) in enumerate(zip(sizes, bases)):
        mine = slab(after(part, *sent), c * half + base + (1 - zh) * size, size)
        theirs = slab(beside[k], (1 - zh) * size, size)
        sent.append((mine.astype(F32) + theirs.astype(F32)).astype(BF16))
        across.append(shift(sent[-1], "zh", 1))
    wide = after(statistic, *sent).reshape(2, 2, width // 2, width)
    near_stat, far_stat = (
        lax.dynamic_index_in_dim(wide, h, 1, keepdims=False).reshape(width, width) for h in (zh, 1 - zh)
    )
    owns = []
    for size, base in zip(sizes, bases):
        owns.append(slab(after(part, *sent, *owns), c * half + base + zh * size, size))
    across[0] = after(across[0], *sent[1:], near_stat, far_stat, *owns)
    totals, lefts, rights = [None, None], [], []
    for k, size in enumerate(sizes):
        theirs = slab(after(beside[k], *sent), zh * size, size)
        pieces = sum_and_split(at, owns[k], theirs, after(across[k], *lefts, *rights))
        lefts, rights = list(pieces[:4]), list(pieces[4:])
        for d in (1, 3, 2):
            lefts[d] = shift(lefts[d], "x", d)
            rights[d] = shift(rights[d], "y", d)
        split = k + 1 == len(sizes)
        parts = gather(lefts, "y", split), gather(rights, "x", split)
        if k:
            parts = lax.optimization_barrier((parts, totals))[0]
        left, right = panels(*parts)
        if k + 1 < len(sizes):
            for i in range(2):
                totals[i] = product(i, (None, None), at, left, right, totals[i], F32)
    own, other = [], []
    for cut in ((1, 0), (None, 1), (0, 0)):
        sibling = product(1, cut, at, left, right, totals[1], BF16)
        other.append(shift(sibling, "c", 1))
        own.append(product(0, cut, at, left, right, totals[0], F32))
    halves = [slice(h * width // 2, (h + 1) * width // 2) for h in range(2)]
    low, high = ((own[0][:, h] + other[0][:, h].astype(F32)).astype(BF16) for h in halves)
    low, high = shift_z(low, -1), shift_z(high, 1)
    above_low, above_high, below_low, below_high = merge(at, own[1], other[1])
    above_low, below_high = shift_z(above_low, 1), shift_z(below_high, -1)
    below_low = shift_z((below_low + low.astype(F32)).astype(BF16), -1)
    above_high = shift_z((above_high + high.astype(F32)).astype(BF16), 1)
    third = width // 2 // sum(THIRDS)
    near = close([n * third for n in THIRDS], own[2], other[2], above_low, below_low, above_high, below_high)
    far, made = [], ()
    for q, n in enumerate(THIRDS):
        beside = shift(near[q], "c", 1)
        far.append(shift(near[q], "zh", 1))
        made = finish(at, 0, sum(THIRDS[:q]), near[q], beside, near_stat, made)
    for q, n in enumerate(THIRDS):
        beside = shift(far[q], "c", 1)
        made = finish(at, 1, sum(THIRDS[:q]), far[q], beside, far_stat, made)
    return tuple(made)


def solution(mesh):
    fine = Mesh(mesh.devices.reshape(2, 2, 4, 2, 4), ("zh", "c", "x", "zl", "y"))
    return jax.shard_map(
        shards,
        mesh=fine,
        in_specs=(P(("zh", "c"), ("x", "zl", "y"), None), P("x", ("zl", "y"))),
        out_specs=(P("x", ("zl", "y")), P("x", ("zl", "y"))),
        check_vma=False,
    )
```

```python
import functools

import jax
import jax.numpy as jnp
from jax import lax
from jax.experimental import pallas as pl
from jax.experimental.pallas import tpu as pltpu
from jax.sharding import Mesh, PartitionSpec as P

BLOCKS = 2, 2, 1, 1
SHARES = (1, 1)
F32, BF16 = jnp.float32, jnp.bfloat16
VMEM = pl.BlockSpec(memory_space=pltpu.VMEM)
SMEM = pl.BlockSpec(memory_space=pltpu.SMEM)
HBM = pl.BlockSpec(memory_space=pltpu.HBM)


def shift(v, axis, step):
    n = lax.axis_size(axis)
    return lax.ppermute(v, axis, [(i, (i + step) % n) for i in range(n)])


def shift_z(v, step):
    return lax.ppermute(v, ("zh", "zl"), [(i, (i + step) % 4) for i in range(4)])


def after(v, *others):
    return lax.optimization_barrier((v, *others))[0]


def slab(v, start, size):
    return lax.dynamic_slice_in_dim(v, start, size)


def params(mib):
    return pltpu.CompilerParams(vmem_limit_bytes=mib * 2**20)


def cost(flops):
    return pl.CostEstimate(flops=flops, bytes_accessed=10**6, transcendentals=0)


def flip(bit, other):
    return bit + other - 2 * bit * other


def sum_kernel(at, own, beside, across, *refs):
    lefts, rights, (total,) = refs[:4], refs[4:8], refs[8:]
    width = own.shape[1] // 8
    c, x, y = at[0], at[1], at[2]
    total[...] = (own[...].astype(F32) + beside[...].astype(F32) + across[...].astype(F32)).astype(BF16)
    for d in range(4):
        for i in range(2):
            block = lax.rem(x + d, 4) * 2 + flip(i, c)
            lefts[d][i] = total[:, pl.ds(pl.multiple_of(block * width, width), width)]
            block = lax.rem(y + d, 4) + 4 * i
            rights[d][i] = total[:, pl.ds(pl.multiple_of(block * width, width), width)]


def sum_and_split(at, own, beside, across):
    rows, width = across.shape[0], across.shape[1] // 8
    piece = jax.ShapeDtypeStruct((2, rows, width), BF16)
    return pl.pallas_call(
        sum_kernel,
        out_shape=[piece] * 8,
        in_specs=[SMEM, VMEM, VMEM, VMEM],
        out_specs=[VMEM] * 8,
        scratch_shapes=[pltpu.VMEM(across.shape, BF16)],
        compiler_params=params(8),
        cost_estimate=cost(10**9),
        name="sum_and_split",
    )(at, own, beside, across)


def piece_at(p, e, d):
    if len(p) == 8:
        return p[2 * e + d // 2].at[d % 2]
    return p[2 + d // 2].at[d % 2] if e == 2 else p[min(e, 2) + 2 * (e == 3)].at[d]


def panel_kernel(*refs):
    n = len(refs) // 2 - 1
    lefts, rights, (left, right) = refs[:n], refs[n : 2 * n], refs[2 * n :]
    rows, width = lefts[0].shape[2:]
    for e in range(4):
        for d in range(4):
            l, r = piece_at(lefts, e, d), piece_at(rights, e, d)
            for i in range(2):
                left[i, pl.ds((e * 4 + d) * rows, rows)] = l[i]
                right[pl.ds((d * 4 + e) * rows, rows), pl.ds(i * width, width)] = r[i]


def panels(lefts, rights):
    rows, width = lefts[0].shape[2:]
    depth = 16 * rows
    return pl.pallas_call(
        panel_kernel,
        out_shape=[
            jax.ShapeDtypeStruct((2, depth, width), BF16),
            jax.ShapeDtypeStruct((depth, 2 * width), BF16),
        ],
        in_specs=[VMEM] * (len(lefts) + len(rights)),
        out_specs=[VMEM] * 2,
        compiler_params=params(2),
        cost_estimate=cost(10**9),
        name="panels",
    )(*lefts, *rights)


def gather(pieces, axis, split):
    if split:
        low, high = jnp.stack(pieces[:2]), jnp.stack(pieces[2:])
        up_low, down_high = shift(low, axis, 1), shift(high, axis, -1)
        up_high, down_low = shift(high, axis, 1), shift(low, axis, -1)
        far_low, far_high = shift(up_low, axis, 1), shift(down_high, axis, -1)
        return [low, high, up_low, up_high, far_low, far_high, down_low, down_high]
    mine = jnp.stack(pieces)
    up, down = shift(mine, axis, 1), shift(mine, axis, -1)
    low, high = shift(up[:2], axis, 1), shift(down[2:], axis, -1)
    return [mine, up, low, high, down]


def merge_kernel(at, own, other, *refs):
    rows, cols = refs[0].shape
    for k, row in enumerate((flip(at[3], at[4]), flip(at[3], 1 - at[4]))):
        rs = pl.ds(pl.multiple_of(row * rows, 16), rows)
        for h in range(2):
            cs = pl.ds(h * cols, cols)
            out = refs[2 * k + h]
            out[...] = (own[rs, cs] + other[rs, cs].astype(F32)).astype(out.dtype)


def merge(at, own, other):
    rows, cols = own.shape
    kinds = BF16, F32, F32, BF16
    return pl.pallas_call(
        merge_kernel,
        out_shape=[jax.ShapeDtypeStruct((rows // 2, cols // 2), kind) for kind in kinds],
        in_specs=[SMEM, VMEM, VMEM],
        out_specs=[VMEM] * 4,
        compiler_params=params(6),
        cost_estimate=cost(10**9),
        name="merge",
    )(at, own, other)


def close_kernel(own, other, above_low, below_low, above_high, below_high, *outs):
    cols = above_low.shape[1]
    first = 0
    for out in outs:
        rs = pl.ds(first, out.shape[0])
        for h, (above, below) in enumerate(((above_low, below_low), (above_high, below_high))):
            cs = pl.ds(h * cols, cols)
            total = own[rs, cs] + other[rs, cs].astype(F32) + above[rs, :].astype(F32) + below[rs, :].astype(F32)
            out[:, cs] = total.astype(BF16)
        first += out.shape[0]


def close(sizes, own, other, *pieces):
    return pl.pallas_call(
        close_kernel,
        out_shape=[jax.ShapeDtypeStruct((size, own.shape[1]), BF16) for size in sizes],
        in_specs=[VMEM] * (2 + len(pieces)),
        out_specs=[VMEM] * len(sizes),
        compiler_params=params(4),
        cost_estimate=cost(10**9),
        name="close",
    )(own, other, *pieces)


def finish_kernel(first, at, here, beside, statistic, *refs):
    gram, following = refs[-2:]
    t, n = pl.program_id(0), pl.num_programs(0) // 2
    rows = gram.shape[0]
    r = lax.rem(t, n)
    there = pl.ds(pl.multiple_of(r * rows, 16), rows)
    old = pl.ds(pl.multiple_of(t // n * (statistic.shape[0] // 2) + (first + r) * rows, 16), rows)
    value = jnp.where(t // n == at[0], here[there, :], beside[there, :]).astype(F32)
    gram[...] = value
    following[...] = 0.95 * statistic[old, :] + 0.05 * value


def finish(at, far, first, here, beside, statistic, made):
    cols = here.shape[1]
    rows = statistic.shape[0] // 2 // sum(BLOCKS)
    n = here.shape[0] // rows
    block = pl.BlockSpec(
        (rows, cols), lambda t, at: ((t // n * 2 + flip(at[3], far)) * sum(BLOCKS) + first + t % n, 0)
    )
    return pl.pallas_call(
        functools.partial(finish_kernel, first),
        grid_spec=pltpu.PrefetchScalarGridSpec(
            num_scalar_prefetch=1,
            grid=(2 * n,),
            in_specs=[VMEM] * 3 + [HBM] * len(made),
            out_specs=[block] * 2,
        ),
        out_shape=[jax.ShapeDtypeStruct((2 * statistic.shape[0], cols), F32)] * 2,
        input_output_aliases={4: 0, 5: 1} if made else {},
        compiler_params=params(8),
        cost_estimate=cost(10**9),
        name="finish",
    )(at, here, beside, statistic, *made)


def product_kernel(i, cut, at, left, right, *refs):
    before, out = refs[:-1], refs[-1]
    width = left.shape[2]
    step = width // 2
    row, col = cut

    def span(base, k, size):
        return pl.ds(k * size, size) if base is None else pl.ds(pl.multiple_of(base * size, size), size)

    for k in range(out.shape[0] // step):
        rs = span(None if row is None else flip(at[3], row), k, step)
        for m in range(out.shape[1] // width):
            cs = span(None if col is None else flip(at[4], col), m, width)
            p = lax.dot_general(left[i, :, rs], right[:, cs], (((0,), (0,)), ((), ())), preferred_element_type=F32)
            for b in before:
                p += b[rs, cs]
            out[pl.ds(k * step, step), pl.ds(m * width, width)] = p.astype(out.dtype)


def product(i, cut, at, left, right, before, dtype):
    rows, cols = left.shape[2] // (1 if cut[0] is None else 2), right.shape[1] // (1 if cut[1] is None else 2)
    given = [left, right] + ([] if before is None else [before])
    return pl.pallas_call(
        functools.partial(product_kernel, i, cut),
        in_specs=[SMEM] + [VMEM] * len(given),
        out_specs=VMEM,
        out_shape=jax.ShapeDtypeStruct((rows, cols), dtype),
        compiler_params=params(6),
        cost_estimate=cost(2 * left.shape[1] * rows * cols),
        name="product",
    )(at, *given)


def shards(grad_parts, statistic):
    part = grad_parts[0]
    width = part.shape[1] // 8
    zh, c, x, zl, y = (lax.axis_index(a) for a in ("zh", "c", "x", "zl", "y"))
    at = jnp.stack([c, x, y, zh, zl]).astype(jnp.int32)
    half = part.shape[0] // 2
    sizes = [half // 2 * s // sum(SHARES) for s in SHARES]
    bases = [2 * sum(sizes[:k]) for k in range(len(sizes))]
    beside, gate = [], part
    for size, base in zip(sizes, bases):
        theirs = slab(gate, (1 - c) * half + base, 2 * size)
        beside.append(shift(theirs, "c", 1))
        gate = after(part, theirs)
    sent, across = [], []
    for k, (size, base) in enumerate(zip(sizes, bases)):
        mine = slab(after(part, *sent), c * half + base + (1 - zh) * size, size)
        theirs = slab(beside[k], (1 - zh) * size, size)
        sent.append((mine.astype(F32) + theirs.astype(F32)).astype(BF16))
        across.append(shift(sent[-1], "zh", 1))
    wide = after(statistic, *sent).reshape(2, 2, width // 2, width)
    near_stat, far_stat = (
        lax.dynamic_index_in_dim(wide, h, 1, keepdims=False).reshape(width, width) for h in (zh, 1 - zh)
    )
    owns = []
    for size, base in zip(sizes, bases):
        owns.append(slab(after(part, *sent, *owns), c * half + base + zh * size, size))
    across[0] = after(across[0], *sent[1:], near_stat, far_stat, *owns)
    totals, lefts, rights = [None, None], [], []
    for k, size in enumerate(sizes):
        theirs = slab(after(beside[k], *sent), zh * size, size)
        pieces = sum_and_split(at, owns[k], theirs, after(across[k], *lefts, *rights))
        lefts, rights = list(pieces[:4]), list(pieces[4:])
        for d in (1, 3, 2):
            lefts[d] = shift(lefts[d], "x", d)
            rights[d] = shift(rights[d], "y", d)
        split = k + 1 == len(sizes)
        parts = gather(lefts, "y", split), gather(rights, "x", split)
        if k:
            parts = lax.optimization_barrier((parts, totals))[0]
        left, right = panels(*parts)
        if k + 1 < len(sizes):
            for i in range(2):
                totals[i] = product(i, (None, None), at, left, right, totals[i], F32)
    own, other = [], []
    for cut in ((1, 0), (None, 1), (0, 0)):
        sibling = product(1, cut, at, left, right, totals[1], BF16)
        other.append(shift(sibling, "c", 1))
        own.append(product(0, cut, at, left, right, totals[0], F32))
    halves = [slice(h * width // 2, (h + 1) * width // 2) for h in range(2)]
    low, high = ((own[0][:, h] + other[0][:, h].astype(F32)).astype(BF16) for h in halves)
    low, high = shift_z(low, -1), shift_z(high, 1)
    above_low, above_high, below_low, below_high = merge(at, own[1], other[1])
    above_low, below_high = shift_z(above_low, 1), shift_z(below_high, -1)
    below_low = shift_z((below_low + low.astype(F32)).astype(BF16), -1)
    above_high = shift_z((above_high + high.astype(F32)).astype(BF16), 1)
    third = width // 2 // sum(BLOCKS)
    near = close([n * third for n in BLOCKS], own[2], other[2], above_low, below_low, above_high, below_high)
    far, made = [], ()
    for q, n in enumerate(BLOCKS):
        beside = shift(near[q], "c", 1)
        far.append(shift(near[q], "zh", 1))
        made = finish(at, 0, sum(BLOCKS[:q]), near[q], beside, near_stat, made)
    for q, n in enumerate(BLOCKS):
        beside = shift(far[q], "c", 1)
        made = finish(at, 1, sum(BLOCKS[:q]), far[q], beside, far_stat, made)
    return tuple(made)


def solution(mesh):
    fine = Mesh(mesh.devices.reshape(2, 2, 4, 2, 4), ("zh", "c", "x", "zl", "y"))
    return jax.shard_map(
        shards,
        mesh=fine,
        in_specs=(P(("zh", "c"), ("x", "zl", "y"), None), P("x", ("zl", "y"))),
        out_specs=(P("x", ("zl", "y")), P("x", ("zl", "y"))),
        check_vma=False,
    )
```
